256 devices in a mesh: grp: 4 (over y), seq: 64 (over z, x, core).
Axes of the slice: x: 4, y: 4, z: 8, core: 2. Of those that a mesh axis runs over, the one named last changes fastest.
Arguments:
- thinker_input: bfloat16 [4, 32, 3584], P(None, 'grp'), as said below
- thinker_gain: float32 [3584], replicated, may hold values from 0.25 to 1.75
- thinker_qkv: bfloat16 [3584, 4608], P('seq'), may hold values from -0.09375 to 0.09375
- thinker_out: bfloat16 [3584, 3584], P('seq'), may hold values from -0.09375 to 0.09375
- talker_proj: bfloat16 [3584, 896], P('seq'), may hold values from -0.09375 to 0.09375
- code_table: bfloat16 [8448, 896], P('seq'), may hold values from -6 to 6
- talker_gain: float32 [896], replicated, may hold values from 0.25 to 1.75
- talker_qkv: bfloat16 [896, 2560], replicated, may hold values from -0.1875 to 0.1875
- talker_out: bfloat16 [1536, 896], replicated, may hold values from -0.15625 to 0.15625
- text_keys: bfloat16 [32, 8192, 512], P('grp', 'seq'), as said below
- text_values: bfloat16 [32, 8192, 512], P('grp', 'seq'), may hold values from -72 to 72
- audio_keys: bfloat16 [32, 8192, 512], P('grp', 'seq'), as said below
- audio_values: bfloat16 [32, 8192, 512], P('grp', 'seq'), may hold values from -72 to 72
- text_len: int32 [32], P('grp'), may hold values from 2 to 8192
- audio_len: int32 [32], P('grp'), may hold values from 2 to 8192
- text_pos: int32 [32, 4], P('grp'), may hold values from 0 to 8195
- audio_pos: int32 [32, 4], P('grp'), may hold values from 0 to 8195
- code_ids: int32 [32, 4], P('grp'), may hold values from 0 to 8447
Outputs:
- thinker_hidden: bfloat16 [4, 32, 3584], P(None, 'grp')
- talker_hidden: bfloat16 [4, 32, 896], P(None, 'grp', 'seq')
The draws below stay inside these ranges and needn't reach their ends.
Inputs may be any that keep to these rules, and one draw needn't show every extreme that they name: Cache positions 0 .. text_len - 1 of a conversation are live. Cache positions 0 .. audio_len - 1 of a conversation are live. `thinker_input`: real-valued, of order one per feature. `text_keys`: real-valued. `audio_keys`: real-valued.
All inputs are finite; a program needn't handle non-finite values.
Results may differ from the reference program's by a relative error of at most 0.028.
Values may be sent and summed in bfloat16 or wider, within the bound.
No kernel may reach another device: no remote copies, remote signals or barrier semaphores. Data moves between devices by JAX's collectives and lax.ppermute only.
A program may use at most 128 MiB of HBM per device.

```python
import math
import jax
import jax.numpy as jnp
import numpy as np
from jax import lax

D = 3584
HQ = 28
HK = 4
HD = 128
TD = 896
AHQ = 12
AHK = 4
AHD = 128
VOCAB = 8448
STEPS = 4
B = 32
TEXT_MAX = 8192
AUDIO_MAX = 8192


def draw_thinker_input(key, part):
    first, second = jax.random.split(jax.random.fold_in(key, 11), 2)
    base = jax.random.normal(first, (STEPS, B, D), jnp.float32)
    columns = jnp.exp(jnp.linspace(jnp.log(0.6), jnp.log(1.8), D))
    rows = jnp.exp(jax.random.uniform(second, (1, B, 1), jnp.float32, jnp.log(0.3), jnp.log(3.0)))
    return jnp.clip(base * rows * columns, -30.0, 30.0).astype(jnp.bfloat16)


def cache_keys(key, batch, count, width):
    first = jax.random.fold_in(key, 0)
    base = 1.5 * jax.random.normal(first, (batch, count, width), jnp.float32)
    return base.astype(jnp.bfloat16)


def draw_text_keys(key, part):
    return cache_keys(jax.random.fold_in(key, 21), B, TEXT_MAX, HK * HD)


def draw_audio_keys(key, part):
    return cache_keys(jax.random.fold_in(key, 31), B, AUDIO_MAX, AHK * AHD)


def touch_ends(drawn, key, low, largest):
    longest = drawn.shape.index(max(drawn.shape))
    spots = []
    for shift in (0, 1):
        where = [jax.random.randint(jax.random.fold_in(key, axis), (), 0, length) for axis, length in enumerate(drawn.shape)]
        where[longest] = (where[longest] + shift) % drawn.shape[longest]
        spots.append(tuple(where))
    return drawn.at[spots[0]].set(low).at[spots[1]].set(largest)


def block_levels(stream_key, shape, cuts, smallest, top_value):
    def one(axis_at, blocks):
        steps = jax.random.uniform(jax.random.fold_in(jax.random.fold_in(stream_key, 6), axis_at), (blocks,), jnp.float32, smallest / len(cuts), top_value / len(cuts))
        return jnp.repeat(jnp.exp(steps), shape[axis_at] // blocks).reshape((-1,) + (1,) * (len(shape) - axis_at - 1))

    gain = one(*cuts[0])
    for cut in cuts[1:]:
        gain = gain * one(*cut)
    return gain


def rank_bounds(amount, slope):
    loads = [(1 << 20) // math.isqrt(rank ** slope) + 1 for rank in range(1, amount + 1)]
    deviation = 1 + sum(loads) // (1 << 30)
    return np.cumsum(np.array([max(1, weight // deviation) for weight in loads]))


def ranked(stream_key, dims, count, lean):
    listing = rank_bounds(count, lean)
    ticket = jax.random.randint(jax.random.fold_in(stream_key, 1), dims, 0, int(listing[count - 1]))
    grade = jnp.searchsorted(jnp.asarray(listing, jnp.int32), ticket, side="right")
    return jax.random.permutation(jax.random.fold_in(stream_key, 2), count)[grade].astype(jnp.int32)


def normal_values(stream_key, extent, scale, reach, cuts=(), held_as=jnp.bfloat16):
    entries = scale * jax.random.normal(stream_key, extent, jnp.float32)
    if cuts:
        entries = entries * block_levels(stream_key, extent, cuts, -0.22, 0.18)
    return jnp.clip(entries, -reach, reach).astype(held_as)


def setup_inputs(seed: int = 0) -> dict:
    key_of = jax.random.split(jax.random.key(seed), 19)
    return {
        "thinker_input": draw_thinker_input(jax.random.fold_in(key_of[18], 71), 0),
        "thinker_gain": jnp.clip(1.0 + 0.15 * jax.random.normal(key_of[1], (D,), jnp.float32), 0.25, 1.75),
        "thinker_qkv": normal_values(key_of[2], (D, D + 2 * HK * HD), D ** -0.5, 0.09375, ((0, 64),)),
        "thinker_out": normal_values(key_of[3], (D, D), D ** -0.5, 0.09375, ((0, 64),)),
        "talker_proj": normal_values(key_of[4], (D, TD), D ** -0.5, 0.09375, ((0, 64),)),
        "code_table": normal_values(key_of[5], (VOCAB, TD), 1.0, 6.0, ((0, 64),)),
        "talker_gain": jnp.clip(1.0 + 0.15 * jax.random.normal(key_of[6], (TD,), jnp.float32), 0.25, 1.75),
        "talker_qkv": normal_values(key_of[7], (TD, AHQ * AHD + 2 * AHK * AHD), TD ** -0.5, 0.1875),
        "talker_out": normal_values(key_of[8], (AHQ * AHD, TD), (AHQ * AHD) ** -0.5, 0.15625),
        "text_keys": draw_text_keys(jax.random.fold_in(key_of[18], 71), 0),
        "text_values": normal_values(key_of[10], (B, TEXT_MAX, HK * HD), 12.0, 72.0, ((0, 4), (1, 64))),
        "audio_keys": draw_audio_keys(jax.random.fold_in(key_of[18], 71), 0),
        "audio_values": normal_values(key_of[12], (B, AUDIO_MAX, AHK * AHD), 12.0, 72.0, ((0, 4), (1, 64))),
        "text_len": touch_ends(jax.random.randint(key_of[13], (B,), 2, TEXT_MAX + 1), jax.random.fold_in(key_of[13], 1), 2, TEXT_MAX).astype(jnp.int32),
        "audio_len": touch_ends(jax.random.randint(key_of[14], (B,), 2, AUDIO_MAX + 1), jax.random.fold_in(key_of[14], 1), 2, AUDIO_MAX).astype(jnp.int32),
        "text_pos": touch_ends(jax.random.randint(key_of[15], (B, STEPS), 0, TEXT_MAX + STEPS), jax.random.fold_in(key_of[15], 1), 0, (TEXT_MAX + STEPS) - 1).astype(jnp.int32),
        "audio_pos": touch_ends(jax.random.randint(key_of[16], (B, STEPS), 0, AUDIO_MAX + STEPS), jax.random.fold_in(key_of[16], 1), 0, (AUDIO_MAX + STEPS) - 1).astype(jnp.int32),
        "code_ids": touch_ends(ranked(key_of[17], (B, STEPS), VOCAB, 2), jax.random.fold_in(key_of[17], 3), 0, VOCAB - 1).astype(jnp.int32),
    }


EPSILON = 1e-06
THETA = 1000000.0
NEGATIVE = -1e+30

def rotate(vectors, positions):
    width = vectors.shape[-1]
    half = width // 2
    freqs = jnp.exp(jnp.arange(half).astype(jnp.float32) * (-2.0 * jnp.log(jnp.float32(THETA)) / width))
    angles = positions.astype(jnp.float32)[:, None] * freqs[None, :]
    cosine = jnp.cos(angles)[:, None, :]
    sine = jnp.sin(angles)[:, None, :]
    first = vectors[..., :half]
    second = vectors[..., half:]
    return jnp.concatenate([first * cosine - second * sine, second * cosine + first * sine], axis=-1)

def attend_all(query, keys, values, new_keys, new_values, lengths, step):
    heads, group, width = query.shape[1:]
    steps = new_keys.shape[1]
    scale = width ** (-0.5)
    fresh_live = jnp.arange(steps) <= step

    def single(item):
        quest, key_cache, value_cache, key_new, value_new, length = item
        count = key_cache.shape[0]
        key_four = key_cache.reshape(count, heads, width).astype(jnp.float32)
        value_four = value_cache.reshape(count, heads, width).astype(jnp.float32)
        quest_wide = quest.astype(jnp.float32)
        cached = jnp.einsum('kgd,tkd->kgt', quest_wide, key_four) * scale
        fresh = jnp.einsum('kgd,skd->kgs', quest_wide, key_new.astype(jnp.float32)) * scale
        live = jnp.arange(count) < length
        cached = jnp.where(live[None, None, :], cached, NEGATIVE)
        fresh = jnp.where(fresh_live[None, None, :], fresh, NEGATIVE)
        peak = jnp.maximum(cached.max(-1), fresh.max(-1))
        weight_cached = jnp.where(live[None, None, :], jnp.exp(cached - peak[..., None]), 0.0)
        weight_fresh = jnp.where(fresh_live[None, None, :], jnp.exp(fresh - peak[..., None]), 0.0)
        total = weight_cached.sum(-1) + weight_fresh.sum(-1)
        narrow_cached = lax.optimization_barrier(weight_cached.astype(jnp.bfloat16)).astype(jnp.float32)
        narrow_fresh = lax.optimization_barrier(weight_fresh.astype(jnp.bfloat16)).astype(jnp.float32)
        summed = jnp.einsum('kgt,tkd->kgd', narrow_cached, value_four)
        summed = summed + jnp.einsum('kgs,skd->kgd', narrow_fresh, value_new.astype(jnp.float32))
        return (summed / total[..., None]).reshape(heads * group * width).astype(jnp.bfloat16)
    return lax.map(single, (query, keys, values, new_keys, new_values, lengths))

def reference(thinker_input, thinker_gain, thinker_qkv, thinker_out, talker_proj, code_table, talker_gain, talker_qkv, talker_out, text_keys, text_values, audio_keys, audio_values, text_len, audio_len, text_pos, audio_pos, code_ids):
    batch = thinker_input.shape[1]
    text_kv = HK * HD
    audio_q = AHQ * AHD
    audio_kv = AHK * AHD
    new_text_keys = jnp.zeros((batch, STEPS, HK, HD), jnp.bfloat16)
    new_text_values = jnp.zeros((batch, STEPS, HK, HD), jnp.bfloat16)
    new_audio_keys = jnp.zeros((batch, STEPS, AHK, AHD), jnp.bfloat16)
    new_audio_values = jnp.zeros((batch, STEPS, AHK, AHD), jnp.bfloat16)
    thinker_rows = []
    talker_rows = []
    for step in range(STEPS):
        inputs = thinker_input[step].astype(jnp.float32)
        scaled = (inputs * thinker_gain).astype(jnp.bfloat16)
        factor = lax.rsqrt(lax.optimization_barrier(jnp.sum(inputs * inputs, axis=-1)) / D + EPSILON)[:, None]
        projected = jnp.dot(scaled, thinker_qkv, preferred_element_type=jnp.float32) * factor
        query = rotate(projected[:, :D].reshape(batch, HQ, HD), text_pos[:, step]).astype(jnp.bfloat16)
        key = rotate(projected[:, D:D + text_kv].reshape(batch, HK, HD), text_pos[:, step]).astype(jnp.bfloat16)
        value = projected[:, D + text_kv:].reshape(batch, HK, HD).astype(jnp.bfloat16)
        new_text_keys = new_text_keys.at[:, step].set(key)
        new_text_values = new_text_values.at[:, step].set(value)
        attended = attend_all(query.reshape(batch, HK, HQ // HK, HD), text_keys, text_values, new_text_keys, new_text_values, text_len, step)
        hidden = (inputs + jnp.dot(attended, thinker_out, preferred_element_type=jnp.float32)).astype(jnp.bfloat16)
        thinker_rows.append(hidden)
        talker_in = code_table[code_ids[:, step]].astype(jnp.float32) + jnp.dot(hidden, talker_proj, preferred_element_type=jnp.float32)
        normed = (talker_in * lax.rsqrt(lax.optimization_barrier(jnp.sum(talker_in * talker_in, axis=-1, keepdims=True)) / TD + EPSILON) * talker_gain).astype(jnp.bfloat16)
        spoken = jnp.dot(normed, talker_qkv, preferred_element_type=jnp.float32)
        audio_query = rotate(spoken[:, :audio_q].reshape(batch, AHQ, AHD), audio_pos[:, step]).astype(jnp.bfloat16)
        audio_key = rotate(spoken[:, audio_q:audio_q + audio_kv].reshape(batch, AHK, AHD), audio_pos[:, step]).astype(jnp.bfloat16)
        audio_value = spoken[:, audio_q + audio_kv:].reshape(batch, AHK, AHD).astype(jnp.bfloat16)
        new_audio_keys = new_audio_keys.at[:, step].set(audio_key)
        new_audio_values = new_audio_values.at[:, step].set(audio_value)
        heard = attend_all(audio_query.reshape(batch, AHK, AHQ // AHK, AHD), audio_keys, audio_values, new_audio_keys, new_audio_values, audio_len, step)
        talker_rows.append((talker_in + jnp.dot(heard, talker_out, preferred_element_type=jnp.float32)).astype(jnp.bfloat16))
    return (jnp.stack(thinker_rows), jnp.stack(talker_rows))
```

```python
import jax
import jax.numpy as jnp
from jax import lax
from jax.experimental import pallas as pl
from jax.experimental.pallas import tpu as pltpu
from jax.sharding import PartitionSpec as P

D = 3584
HQ = 28
HK = 4
HD = 128
TD = 896
AHQ = 12
AHK = 4
AHD = 128
SEQ = "seq"
EPSILON = 1e-06
THETA = 1000000.0
NEGATIVE = -1e30
DEV = 64
ROWS = 32
BATCH = 8
STEPS = 4
FT = 56
FA = 24
CT = 14
INTERPRET = False

f32 = jnp.float32
bf16 = jnp.bfloat16
VM = pltpu.VMEM


def call(kernel, outs, scratch=(), name=None, scalars=1, count=0):
    specs = [pl.BlockSpec(memory_space=pltpu.SMEM)] * scalars + [pl.BlockSpec(memory_space=VM)] * count
    many = isinstance(outs, (tuple, list))
    return pl.pallas_call(
        kernel,
        out_shape=outs,
        in_specs=specs,
        out_specs=[pl.BlockSpec(memory_space=VM)] * len(outs) if many else pl.BlockSpec(memory_space=VM),
        scratch_shapes=list(scratch),
        name=name,
        interpret=INTERPRET,
    )


def iota(shape, axis):
    return lax.broadcasted_iota(jnp.int32, shape, axis)


def roll(x, shift):
    shift = shift % x.shape[1]
    return x if shift == 0 else pltpu.roll(x, shift, 1)


def mm(a, b):
    return jnp.dot(a, b, preferred_element_type=f32)


def pack(out_ref, block, extra, width, groups):
    span = 128 // groups
    high = ROWS // groups
    lane = iota((ROWS, 128), 1)
    for j in range(DEV):
        first, off = divmod(width * j, 128)
        n0 = min(width, 128 - off)
        tile = roll(block(first), -off)
        if n0 < width:
            tile = jnp.where(lane < n0, tile, roll(block(first + 1), n0))
        if extra is None:
            tile = jnp.where(lane < width, tile, 0.0)
        else:
            tail = extra(first)
            if n0 < width:
                tail = tail + roll(extra(first + 1), 3)
            tile = jnp.where(lane < width, tile, tail)
        out = tile[0:high]
        for g in range(1, groups):
            out = out + roll(tile[g * high : (g + 1) * high], g * span)
        out_ref[j] = out.astype(bf16)


def unpack(tile, groups):
    span = 128 // groups
    return jnp.concatenate([roll(tile, -g * span) for g in range(groups)], axis=0)


def attend(q_of, kn_of, vn_of, keys_ref, values_ref, limit, dev, group, o_ref, e_ref, width):
    high = group * ROWS
    row = iota((high, 128), 0)
    lane = iota((high, 128), 1)
    conv = row & 7
    lim = jnp.broadcast_to(limit[None], (group * STEPS, BATCH, 128)).reshape(high, 128)
    live = lane < lim
    frow = iota((high, ROWS), 0)
    fcol = iota((high, ROWS), 1)
    reach = jnp.where(dev == 0, (frow >> 3) & 3, -1)
    fresh_live = ((frow & 7) == (fcol & 7)) & ((fcol >> 3) <= reach)
    scale = HD**-0.5
    for k in range(HK):
        q = q_of(k)
        keys = keys_ref[:, :, 128 * k : 128 * k + 128].reshape(BATCH * 128, 128)
        values = values_ref[:, :, 128 * k : 128 * k + 128].reshape(BATCH * 128, 128)
        every = lax.dot_general(q, keys, (((1,), (1,)), ((), ())), preferred_element_type=f32)
        s = every[:, 0:128]
        for b in range(1, BATCH):
            s = jnp.where(conv == b, every[:, 128 * b : 128 * b + 128], s)
        f = lax.dot_general(q, kn_of(k), (((1,), (1,)), ((), ())), preferred_element_type=f32)
        s = jnp.where(live, s * scale, NEGATIVE)
        f = jnp.where(fresh_live, f * scale, NEGATIVE)
        m = jnp.maximum(jnp.max(s, axis=1, keepdims=True), jnp.max(f, axis=1, keepdims=True))
        w = jnp.where(live, jnp.exp(s - m), 0.0)
        wf = jnp.where(fresh_live, jnp.exp(f - m), 0.0)
        total = jnp.sum(w, axis=1, keepdims=True) + jnp.sum(wf, axis=1, keepdims=True)
        wide = jnp.concatenate(
            [jnp.where(conv == b, w, 0.0).astype(bf16) for b in range(BATCH)], axis=1
        )
        o = mm(wide, values) + mm(wf.astype(bf16), vn_of(k))
        some = total > 0.0
        safe = jnp.where(some, total, 1.0)
        o = o * (1.0 / safe)
        lse = jnp.where(some, m + jnp.log(safe), NEGATIVE)
        hi = lse.astype(bf16).astype(f32)
        rest = lse - hi
        mid = rest.astype(bf16).astype(f32)
        low = rest - mid
        e = jnp.where(
            lane == width, hi, jnp.where(lane == width + 1, mid, jnp.where(lane == width + 2, low, 0.0))
        )
        for g in range(group):
            o_ref[k * group + g] = o[ROWS * g : ROWS * g + ROWS]
            e_ref[k * group + g] = e[ROWS * g : ROWS * g + ROWS]


def merged(x_ref, dev, width, groups):
    high = ROWS // groups
    span = 128 // groups
    n0 = jnp.minimum(width, 128 - (width * dev) % 128)
    a = iota((128, 128), 0)
    c = iota((128, 128), 1)
    start = jnp.where((c & (span - 1)) < n0, width, width + 3)
    delta = (a & (span - 1)) - start
    pick = ((a // span) == (c // span)) & (delta >= 0) & (delta < 3)
    pick = jnp.where(pick, 1.0, 0.0).astype(bf16)
    x = x_ref[...].astype(f32)
    lse = mm(x.reshape(DEV * high, 128).astype(bf16), pick).reshape(DEV, high, 128)
    peak = jnp.max(lse, axis=0)
    w = jnp.exp(lse - peak[None])
    return jnp.sum(w * x, axis=0) / jnp.sum(w, axis=0)


def k_qkv(dev_ref, x_ref, g_ref, w_ref, out_ref):
    scaled = (x_ref[...].astype(f32) * g_ref[...]).astype(bf16)[:, 0:FT]
    for h in range(HQ + 2 * HK):
        y = mm(scaled, w_ref[:, 128 * h : 128 * h + 128])
        for s in range(STEPS):
            j, i = divmod(4 * h + s, 3)
            out_ref[j, 8 * i : 8 * i + 8, :] = y[8 * s : 8 * s + 8].astype(bf16)
    for j in range(48, DEV):
        out_ref[j] = jnp.zeros((24, 128), bf16)


def k_rotate(dev_ref, x_ref, c_ref, s_ref, r_ref, out_ref):
    y = jnp.sum(x_ref[...].astype(f32), axis=0)
    parts = []
    for i in range(3):
        u = 3 * dev_ref[0] + i
        step = u & 3
        plain = u >= 4 * (HQ + HK)
        v = y[8 * i : 8 * i + 8]
        c = jnp.where(plain, jnp.ones((8, 128), f32), c_ref[step])
        s = jnp.where(plain, jnp.zeros((8, 128), f32), s_ref[step])
        parts.append((v * c + roll(v, 64) * s) * r_ref[step])
    z = jnp.concatenate(parts, axis=0).astype(bf16)
    out_ref[...] = jnp.broadcast_to(z[None], (DEV, 24, 128))


def k_text(dev_ref, q_ref, keys_ref, values_ref, limit_ref, out_ref, o_ref, e_ref):
    g = HQ // HK
    attend(
        lambda k: q_ref[ROWS * g * k : ROWS * g * (k + 1), :],
        lambda k: q_ref[ROWS * (HQ + k) : ROWS * (HQ + k + 1), :],
        lambda k: q_ref[ROWS * (HQ + HK + k) : ROWS * (HQ + HK + k + 1), :],
        keys_ref,
        values_ref,
        limit_ref[...],
        dev_ref[0],
        g,
        o_ref,
        e_ref,
        FT,
    )
    pack(out_ref, lambda h: o_ref[h], lambda h: e_ref[h], FT, 2)


def k_out(dev_ref, x_ref, w_ref, out_ref):
    att = unpack(merged(x_ref, dev_ref[0], FT, 2), 2).astype(bf16)[:, 0:FT]
    y = mm(att, w_ref[...])
    pack(out_ref, lambda h: y[:, 128 * h : 128 * h + 128], None, FT, 2)


def k_bridge(dev_ref, x_ref, in_ref, proj_ref, ids_ref, table_ref, hid_ref, out_ref):
    mine = in_ref[...].astype(f32)
    mine = mine[0:16] + roll(mine[16:32], 64)
    hid = (jnp.sum(x_ref[...].astype(f32), axis=0) + mine).astype(bf16)
    hid_ref[...] = hid
    rows = unpack(hid.astype(f32), 2).astype(bf16)[:, 0:FT]
    table = table_ref.shape[0]
    picked = ids_ref[...] - dev_ref[0] * table == iota((ROWS, table), 1)
    picked = jnp.where(picked, 1.0, 0.0).astype(bf16)
    y = mm(rows, proj_ref[...]) + mm(picked, table_ref[...])
    for s in range(STEPS):
        for n in range(TD // 128):
            out_ref[s * 7 + n] = y[8 * s : 8 * s + 8, 128 * n : 128 * n + 128].astype(bf16)
    for j in range(28, DEV):
        out_ref[j] = jnp.zeros((8, 128), bf16)


def k_spread(dev_ref, x_ref, hid_ref, out_ref):
    y = jnp.sum(x_ref[...].astype(f32), axis=0).astype(bf16)
    out_ref[:, 0:16, :] = jnp.broadcast_to(hid_ref[...][None], (DEV, 16, 128))
    out_ref[:, 16:24, :] = jnp.broadcast_to(y[None], (DEV, 8, 128))


def talker_rows(x_ref):
    return jnp.concatenate(
        [
            jnp.concatenate([x_ref[7 * s + n, 16:24, :].astype(f32) for n in range(7)], axis=1)
            for s in range(STEPS)
        ],
        axis=0,
    )


def k_audio(
    dev_ref, x_ref, gain_ref, w_ref, c_ref, s_ref, keys_ref, values_ref, limit_ref,
    out_ref, hidden_ref, q_ref, o_ref, e_ref,
):
    t = talker_rows(x_ref)
    factor = lax.rsqrt(jnp.sum(t * t, axis=1, keepdims=True) / TD + EPSILON)
    normed = (t * factor * gain_ref[...]).astype(bf16)
    c = c_ref[...].reshape(ROWS, 128)
    s = s_ref[...].reshape(ROWS, 128)
    y = mm(normed, w_ref[...])
    for h in range(AHQ + 2 * AHK):
        v = y[:, 128 * h : 128 * h + 128]
        if h < AHQ + AHK:
            v = v * c + roll(v, 64) * s
        q_ref[ROWS * h : ROWS * h + ROWS, :] = v.astype(bf16)
    g = AHQ // AHK
    attend(
        lambda k: q_ref[ROWS * g * k : ROWS * g * (k + 1), :],
        lambda k: q_ref[ROWS * (AHQ + k) : ROWS * (AHQ + k + 1), :],
        lambda k: q_ref[ROWS * (AHQ + AHK + k) : ROWS * (AHQ + AHK + k + 1), :],
        keys_ref,
        values_ref,
        limit_ref[...],
        dev_ref[0],
        g,
        o_ref,
        e_ref,
        FA,
    )
    pack(out_ref, lambda h: o_ref[h], lambda h: e_ref[h], FA, 4)
    lane = iota((16, 128), 1)
    for h in range(HQ):
        left = jnp.zeros((16, 128), f32)
        right = jnp.zeros((16, 128), f32)
        for j in range(128 * h // FT, (128 * h + 127) // FT + 1):
            at = FT * j - 128 * h
            tile = x_ref[j, 0:16, :].astype(f32)
            inside = (lane >= at) & (lane < at + FT)
            left = jnp.where(inside, roll(tile, at), left)
            right = jnp.where(inside, roll(tile, at - 64), right)
        hidden_ref[0:16, 128 * h : 128 * h + 128] = left.astype(bf16)
        hidden_ref[16:32, 128 * h : 128 * h + 128] = right.astype(bf16)


def k_heard(dev_ref, x_ref, t_ref, w_ref, out_ref):
    heard = unpack(merged(x_ref, dev_ref[0], FA, 4), 4).astype(bf16)[:, 0:FA]
    y = mm(heard, w_ref[...])
    y = y + jnp.where(dev_ref[0] == 0, talker_rows(t_ref), 0.0)
    pack(out_ref, lambda h: y[:, 128 * h : 128 * h + 128], None, CT, 4)


def k_last(dev_ref, x_ref, out_ref):
    y = jnp.sum(x_ref[...].astype(f32), axis=0)
    for s in range(STEPS):
        out_ref[s] = roll(y, -32 * s)[:, 0:CT].astype(bf16)


def swap(x):
    return lax.all_to_all(x, SEQ, 0, 0, tiled=True)


def tables(positions):
    half = HD // 2
    freqs = jnp.exp(jnp.arange(half).astype(f32) * (-2.0 * jnp.log(f32(THETA)) / HD))
    angles = positions.T.astype(f32)[:, :, None] * freqs[None, None, :]
    cosine = jnp.cos(angles)
    sine = jnp.sin(angles)
    return (
        jnp.concatenate([cosine, cosine], axis=-1),
        jnp.concatenate([-sine, sine], axis=-1),
    )


def body(
    thinker_input,
    thinker_gain,
    thinker_qkv,
    thinker_out,
    talker_proj,
    code_table,
    talker_gain,
    talker_qkv,
    talker_out,
    text_keys,
    text_values,
    audio_keys,
    audio_values,
    text_len,
    audio_len,
    text_pos,
    audio_pos,
    code_ids,
):
    index = lax.axis_index(SEQ)
    dev = index.reshape(1).astype(jnp.int32)
    shape = jax.ShapeDtypeStruct
    count = text_keys.shape[1]
    x = thinker_input.reshape(ROWS, D)
    mine = jnp.pad(lax.dynamic_slice_in_dim(x, index * FT, FT, 1), ((0, 0), (0, 128 - FT)))
    gain = jnp.pad(lax.dynamic_slice_in_dim(thinker_gain, index * FT, FT, 0), (0, 128 - FT))
    partial_qkv = call(k_qkv, shape((DEV, 24, 128), bf16), name="k_qkv", count=3)(
        dev, mine, gain.reshape(1, 128), thinker_qkv
    )
    wide = thinker_input.astype(f32)
    factor = lax.rsqrt(jnp.sum(wide * wide, axis=-1, keepdims=True) / D + EPSILON)
    factor = jnp.broadcast_to(factor, (STEPS, BATCH, 128))
    cosine, sine = tables(text_pos)
    audio_cosine, audio_sine = tables(audio_pos)
    text_limit = jnp.broadcast_to((text_len - index * count)[:, None], (BATCH, 128))
    audio_limit = jnp.broadcast_to((audio_len - index * count)[:, None], (BATCH, 128))
    ids = code_ids.T.reshape(ROWS, 1)
    out_rows = lax.dynamic_slice_in_dim(talker_out, index * FA, FA, 0)

    q = call(k_rotate, shape((DEV, 24, 128), bf16), name="k_rotate", count=4)(
        dev, swap(partial_qkv), cosine, sine, factor
    )
    q = swap(q).reshape(DEV * 24, 128)
    parts = call(
        k_text,
        shape((DEV, 16, 128), bf16),
        [VM((HQ, ROWS, 128), f32), VM((HQ, ROWS, 128), f32)],
        name="k_text",
        count=4,
    )(dev, q, text_keys, text_values, text_limit)
    parts = call(k_out, shape((DEV, 16, 128), bf16), name="k_out", count=2)(
        dev, swap(parts), thinker_out
    )
    hid, pieces = call(
        k_bridge, (shape((16, 128), bf16), shape((DEV, 8, 128), bf16)), name="k_bridge", count=5
    )(dev, swap(parts), mine, talker_proj, ids, code_table)
    both = call(k_spread, shape((DEV, 24, 128), bf16), name="k_spread", count=2)(
        dev, swap(pieces), hid
    )
    both = swap(both)
    parts, hidden = call(
        k_audio,
        (shape((DEV, 8, 128), bf16), shape((ROWS, D), bf16)),
        [
            VM(((AHQ + 2 * AHK) * ROWS, 128), bf16),
            VM((AHQ, ROWS, 128), f32),
            VM((AHQ, ROWS, 128), f32),
        ],
        name="k_audio",
        count=8,
    )(
        dev, both, talker_gain.reshape(1, TD), talker_qkv, audio_cosine, audio_sine,
        audio_keys, audio_values, audio_limit,
    )
    parts = call(k_heard, shape((DEV, 8, 128), bf16), name="k_heard", count=3)(
        dev, swap(parts), both, out_rows
    )
    talker = call(k_last, shape((STEPS, BATCH, CT), bf16), name="k_last", count=1)(
        dev, swap(parts)
    )
    return hidden.reshape(STEPS, BATCH, D), talker


def solution(mesh):
    placed = (
        P(None, "grp", None),
        P(),
        P(SEQ, None),
        P(SEQ, None),
        P(SEQ, None),
        P(SEQ, None),
        P(),
        P(),
        P(),
        P("grp", SEQ, None),
        P("grp", SEQ, None),
        P("grp", SEQ, None),
        P("grp", SEQ, None),
        P("grp"),
        P("grp"),
        P("grp", None),
        P("grp", None),
        P("grp", None),
    )
    return jax.shard_map(
        body,
        mesh=mesh,
        in_specs=placed,
        out_specs=(P(None, "grp", None), P(None, "grp", SEQ)),
        check_vma=False,
    )
```
